32 devices in a mesh: node: 8 (over z, x), local: 4 (over y, core).
Axes of the slice: x: 2, y: 2, z: 4, core: 2. Of those that a mesh axis runs over, the one named last changes fastest.
Arguments:
- gate_pre: bfloat16 [3584, 15360], P('node', 'local'), may hold values from -6 to 6
- up_pre: bfloat16 [3584, 15360], P('node', 'local'), may hold values from -6 to 6
- out_grad: bfloat16 [3584, 4096], P('node', 'local'), may hold values from -6 to 6
Outputs:
- weight_grad: float32 [15360, 4096], P('local', 'node')
The draws below stay inside these ranges and needn't reach their ends.
All inputs are finite; a program needn't handle non-finite values.
Results may differ from the reference program's by a relative error of at most 0.015.
Values may be sent and summed in bfloat16 or wider, within the bound.
A program may use at most 128 MiB of HBM per device.

```python
import jax
import jax.numpy as jnp
from jax import lax

D = 4096
BUCKET = 15360
TOK_DEV = 448
TOKENS = 3584
N_NODE = 8


def strengthened(result, own_key, source, target, parts, factor):
    def block_of(axis_at):
        return (jnp.arange(result.shape[axis_at]) // (result.shape[axis_at] // parts)).reshape((-1,) + (1,) * (result.ndim - 1 - axis_at))

    near = jax.random.permutation(own_key, parts)[block_of(target)]
    other_side = (block_of(target) + parts // 2) % parts
    return jnp.where((block_of(source) == near) | (block_of(source) == other_side), factor * result, result)


def shard_levels(rng, extent, cuts, low, largest):
    def one(axis_at, parts):
        steps = jax.random.uniform(jax.random.fold_in(jax.random.fold_in(rng, 6), axis_at), (parts,), jnp.float32, low / len(cuts), largest / len(cuts))
        return jnp.repeat(jnp.exp(steps), extent[axis_at] // parts).reshape((-1,) + (1,) * (len(extent) - axis_at - 1))

    factor_of = one(*cuts[0])
    for cut in cuts[1:]:
        factor_of = factor_of * one(*cut)
    return factor_of


def centred(rng, shape, spread, most, pieces=(), held_as=jnp.bfloat16):
    values = spread * jax.random.normal(rng, shape, jnp.float32)
    if pieces:
        values = values * shard_levels(rng, shape, pieces, -0.22, 0.18)
    return jnp.clip(values, -most, most).astype(held_as)


def noise_with(key, shape, width, reach, cuts, heavy, dtype=jnp.bfloat16):
    result = width * jax.random.normal(key, shape, jnp.float32)
    if cuts:
        result = result * shard_levels(key, shape, cuts, -0.22, 0.18)
    return jnp.clip(strengthened(result, jax.random.fold_in(key, 3), *heavy), -reach, reach).astype(dtype)


def setup_inputs(seed: int = 0) -> dict:
    key_of = jax.random.split(jax.random.key(seed), 4)
    gate_pre = centred(key_of[0], (TOKENS, BUCKET), 1.0, 6.0, ((0, 8), (1, 4)))
    up_pre = centred(key_of[1], (TOKENS, BUCKET), 1.0, 6.0, ((0, 8), (1, 4)))
    out_grad = noise_with(key_of[2], (TOKENS, D), 1.0, 6.0, ((0, 8), (1, 4)), (0, 1, 8, 2.0))
    return {"gate_pre": gate_pre, "up_pre": up_pre, "out_grad": out_grad}


def reference(gate_pre, up_pre, out_grad):
    averaging = 1.0 / N_NODE

    def advance(accumulated, inputs):
        gate_block, up_block, grad_block = inputs
        gate_float = gate_block.astype(jnp.float32)
        activated = gate_float * jax.nn.sigmoid(gate_float)
        hidden = (activated * up_block.astype(jnp.float32)).astype(jnp.bfloat16)
        product = lax.dot_general(hidden.astype(jnp.float32), grad_block.astype(jnp.float32), (((0,), (0,)), ((), ())), preferred_element_type=jnp.float32)
        term = (product * averaging).astype(jnp.bfloat16)
        return accumulated + term.astype(jnp.float32), None

    initial = jnp.zeros((BUCKET, D), jnp.float32)
    stacked = (gate_pre.reshape(N_NODE, TOK_DEV, BUCKET), up_pre.reshape(N_NODE, TOK_DEV, BUCKET), out_grad.reshape(N_NODE, TOK_DEV, D))
    total, unused = lax.scan(advance, initial, stacked)
    return total
```

```python
import functools

import jax
import jax.numpy as jnp
from jax import lax
from jax.experimental import pallas as pl
from jax.experimental.pallas import tpu as pltpu
from jax.sharding import PartitionSpec as P

TILE = 128
LAG = 12
EARLY = 4
STRIPS = 2


def strips_of(width):
    return next(n for n in (STRIPS, 2, 1) if width % (n * TILE) == 0)


def kernel(
    n_node, n_local, gate_hbm, up_hbm, grad_hbm, out_ref,
    gate, up, own, hidden, grads, going, coming, giving,
    in_sem, own_sem, l_send, l_recv, g_sem, twin_sem, h_send, h_recv, p_sem, o_send, o_recv,
):
    wide, deep, tall = n_node // n_local, n_local, n_local // 2
    layers = deep // 2
    node, local = lax.axis_index("node"), lax.axis_index("local")
    z, x, y, c = node // wide, node % wide, local // 2, local % 2
    side = z // layers
    tokens, units = gate.shape
    width = out_ref.shape[1]
    count = units // TILE
    strips = strips_of(width)
    strip = width // strips
    slots = layers * wide
    averaging = 1.0 / n_node

    def depth(zz):
        return jnp.where(zz < layers, layers - 1 - zz, zz - layers)

    def layer(half, d):
        return jnp.where(half == 0, layers - 1 - d, layers + d)

    mine = depth(z)
    inside = mine == 0
    outside = jnp.logical_not(inside)
    inner_z = layer(side, 0)
    mirror = (layer(1 - side, 0) * wide + x, local)
    twin = (node, y * 2 + 1 - c)

    def device(zz, xx, yy, cc):
        return (zz * wide + xx, yy * 2 + cc)

    def beside(i):
        return (x + i) % wide

    def slot_of(d, xx):
        return d * wide + xx

    my_slot = slot_of(mine, x)

    def rows(slot):
        return pl.ds(pl.multiple_of(slot * tokens, 16), tokens)

    def chunk(k):
        return pl.ds(pl.multiple_of(k * TILE, TILE), TILE)

    def remote(source, target, send, recv, where):
        return pltpu.make_async_remote_copy(
            src_ref=source, dst_ref=target, send_sem=send, recv_sem=recv,
            device_id=where, device_id_type=pl.DeviceIdType.MESH,
        )

    def loads(k):
        return [
            pltpu.make_async_copy(gate_hbm.at[:, chunk(k)], gate.at[:, chunk(k)], in_sem.at[k, 0]),
            pltpu.make_async_copy(up_hbm.at[:, chunk(k)], up.at[:, chunk(k)], in_sem.at[k, 1]),
        ]

    own_load = pltpu.make_async_copy(grad_hbm, own, own_sem)
    own_load.start()
    for copy in loads(0):
        copy.start()

    @pl.loop(1, count)
    def _(k):
        for copy in loads(k):
            copy.start()

    barrier = pltpu.get_barrier_semaphore()

    def greet(target):
        pl.semaphore_signal(
            barrier, inc=1, device_id=target, device_id_type=pl.DeviceIdType.MESH
        )

    ring = [(i, j, m) for i in range(wide) for j in range(tall) for m in range(2)]

    @pl.when(inside)
    def _():
        greet(mirror)
        for d in range(layers):
            for i, j, m in ring:
                if (d, i, j, m) != (0, 0, 0, 0):
                    greet(device(layer(side, d), beside(i), (y + j) % tall, (c + m) % 2))
        pl.semaphore_wait(barrier, layers * len(ring))

    layer_mates = [(i, j) for i in range(wide) for j in range(tall) if (i, j) != (0, 0)]

    @pl.when(outside)
    def _():
        for i, j, m in ring:
            greet(device(inner_z, beside(i), (y + j) % tall, (c + m) % 2))
        for i, j in layer_mates:
            greet(device(z, beside(i), (y + j) % tall, c))
        pl.semaphore_wait(barrier, len(ring) + len(layer_mates))

    half = tall // 2

    def row_of(near, i):
        low, high = i, tall - 1 - i
        return jnp.where((side == 0) == near, low, high)

    def entry(near, i, cc):
        return (layers if near else 0) + depth(row_of(near, i) * 2 + cc)

    own_near = jnp.where(y >= half, 1, 0) == side
    own_low = y < half
    own_at = jnp.where(own_near, half, 0) + jnp.where(own_low, y, tall - 1 - y)
    own_entry = jnp.where(own_near, layers, 0) + depth(y * 2 + c)

    def share_source(t, i, held):
        return held.at[:, pl.ds(pl.multiple_of(beside(i) * width + t * strip, TILE), strip)]

    def share_target(t):
        return grads.at[own_entry, rows(my_slot), pl.ds(t * strip, strip)]

    def share(t, i, j):
        return remote(
            share_source(t, i, own), share_target(t), l_send.at[t, i * tall + j], l_recv.at[own_at, t, x],
            device(z, beside(i), (y + j) % tall, c),
        )

    def keep(t):
        return pltpu.make_async_copy(share_source(t, 0, grad_hbm), share_target(t), l_recv.at[own_at, t, x])

    own_load.wait()
    for t in range(strips):
        for i, j in layer_mates:
            share(t, i, j).start()
    for t in range(strips):
        keep(t).start()

    def layer_rows(d):
        return pl.ds(pl.multiple_of(d * (wide * tokens), 16), wide * tokens)

    def shared(near, i, t):
        for xx in range(wide):
            part = grads.at[entry(near, i, c), rows(slot_of(mine, xx)), pl.ds(t * strip, strip)]
            pltpu.make_async_copy(part, part, l_recv.at[near * half + i, t, xx]).wait()

    def g_copy(near, i, t, d):
        part = grads.at[entry(near, i, c), layer_rows(d), pl.ds(t * strip, strip)]
        at = near * half + i
        return remote(
            part, part, g_sem.at[at, t, d - 1, 0], g_sem.at[at, t, d - 1, 1],
            device(inner_z, x, y, c),
        )

    def each_depth(act):
        for d in range(1, layers):
            @pl.when(mine == d)
            def _():
                act(d)

    def g_start(near, t):
        for i in range(half):
            shared(near, i, t)
            each_depth(lambda d: g_copy(near, i, t, d).start())

    def twin_copy(near, i, t, cc):
        part = grads.at[entry(near, i, cc), :, pl.ds(t * strip, strip)]
        at = near * half + i
        return remote(part, part, twin_sem.at[at, t, 0], twin_sem.at[at, t, 1], twin)

    def g_pass(near, t):
        for i in range(half):
            shared(near, i, t)
            for d in range(1, layers):
                g_copy(near, i, t, d).wait_recv()
            twin_copy(near, i, t, c).start()

    def g_passed(near, t):
        for i in range(half):
            twin_copy(near, i, t, 1 - c).wait_recv()

    step = next(b for b in (128, 112, 96, 64, 32, 16) if tokens % b == 0)

    def activate(k):
        for copy in loads(k):
            copy.wait()
        at = chunk(k)
        for first in range(0, tokens, step):
            g = gate[pl.ds(first, step), at].astype(jnp.float32)
            u = up[pl.ds(first, step), at].astype(jnp.float32)
            value = g * jax.nn.sigmoid(g) * u
            into = pl.ds(pl.multiple_of(my_slot * tokens + first, 16), step)
            hidden[into, at] = value.astype(hidden.dtype)

    def h_copy(k, slot, index, where):
        part = hidden.at[rows(slot), chunk(k)]
        return remote(part, part, h_send.at[k, index], h_recv.at[k, slot], where)

    def here(k, i):
        return h_copy(k, my_slot, i, device(z, beside(i), y, c))

    def inward(k):
        return h_copy(k, my_slot, 0, device(inner_z, x, y, c))

    def relay_out(k, i):
        return h_copy(k, slot_of(mine, beside(i)), wide + i - 1, device(inner_z, x, y, c))

    def relay_in(k, d, i):
        return h_copy(k, slot_of(d, x), d * wide + i, device(z, beside(i), y, c))

    def early(k):
        return k % 3 == 2

    def late(k):
        return k % 3 != 2

    def send_in(k):
        activate(k)
        for i in range(1, wide):
            here(k, i).start()

    def send_out(k):
        activate(k)
        inward(k).start()

        @pl.when(early(k))
        def _():
            for i in range(1, wide):
                here(k, i).start()

    def pass_out(k):
        @pl.when(early(k))
        def _():
            for i in range(1, wide):
                h_copy(k, slot_of(mine, beside(i)), 0, twin).wait_recv()
                relay_out(k, i).start()

    def pass_in(k):
        for d in range(1, layers):
            h_copy(k, slot_of(d, x), 0, twin).wait_recv()

            @pl.when(late(k))
            def _():
                for i in range(1, wide):
                    relay_in(k, d, i).start()

    def gathered(k):
        for d in range(layers):
            for i in range(1, wide):
                h_copy(k, slot_of(d, beside(i)), 0, twin).wait_recv()

    def product(k, index, at):
        return lax.dot_general(
            hidden[:, chunk(k)], grads[index, :, at], (((0,), (0,)), ((), ())),
            preferred_element_type=jnp.float32,
        ) * averaging

    def p_copy(k, index, at):
        return remote(
            going.at[index, chunk(k), at], coming.at[index, chunk(k), at],
            p_sem.at[k, index, 0], p_sem.at[k, index, 1], mirror,
        )

    whole = pl.ds(0, width)

    def far(k, i, cc, at):
        index = entry(False, i, cc)
        going[index, chunk(k), at] = product(k, index, at).astype(going.dtype)
        p_copy(k, index, at).start()

    def o_copy(k, d):
        return remote(
            giving.at[d - 1, chunk(k)], out_ref.at[chunk(k)],
            o_send.at[k, d - 1], o_recv.at[k], device(layer(side, d), x, y, c),
        )

    def near(k):
        for d in reversed(range(layers)):
            p_copy(k, d, whole).wait_recv()
            total = product(k, layers + d, whole) + coming[d, chunk(k)].astype(jnp.float32)
            if d:
                giving[d - 1, chunk(k)] = total.astype(giving.dtype)
                o_copy(k, d).start()
            else:
                out_ref[chunk(k)] = total.astype(out_ref.dtype)

    first_c = 1 - side

    @pl.when(inside)
    def _():
        send_in(0)
        send_in(1)
        pass_in(0)
        g_pass(False, 0)
        for t in range(strips):
            if t:
                g_pass(False, t)
            for k in range(EARLY):
                if t == 0:
                    send_in(k + 2)
                    pass_in(k + 1)
                    gathered(k)
                for i in range(half):
                    far(k, i, c, pl.ds(t * strip, strip))
                if k == 0:
                    g_passed(False, t)
                for i in range(half):
                    far(k, i, 1 - c, pl.ds(t * strip, strip))

        def body(k):
            @pl.when(k + 2 < count)
            def _():
                send_in(k + 2)

            @pl.when(k + 1 < count)
            def _():
                pass_in(k + 1)

            gathered(k)
            for i in range(half):
                far(k, i, first_c, whole)
                far(k, i, 1 - first_c, whole)

        @pl.loop(EARLY, LAG)
        def _(k):
            body(k)

        for t in range(strips):
            g_pass(True, t)
        for t in range(strips):
            g_passed(True, t)

        @pl.loop(LAG, count)
        def _(k):
            body(k)
            near(k - LAG)

        @pl.loop(count - LAG, count)
        def _(k):
            near(k)

        @pl.loop(0, count)
        def _(k):
            for i in range(1, wide):
                here(k, i).wait_send()

            @pl.when(late(k))
            def _():
                for d in range(1, layers):
                    for i in range(1, wide):
                        relay_in(k, d, i).wait_send()

            for d in range(layers):
                p_copy(k, d, whole).wait_send()
            for d in range(1, layers):
                o_copy(k, d).wait_send()

        for near_too in (False, True):
            for t in range(strips):
                for i in range(half):
                    twin_copy(near_too, i, t, c).wait_send()

    @pl.when(outside)
    def _():
        send_out(0)
        g_start(False, 0)
        send_out(1)
        pass_out(0)
        for t in range(1, strips):
            g_start(False, t)

        @pl.loop(2, count)
        def _(k):
            for t in range(strips):
                @pl.when(k == EARLY + 2 + 2 * t)
                def _():
                    g_start(True, t)

            send_out(k)
            pass_out(k - 1)

        pass_out(count - 1)

        @pl.loop(0, count)
        def _(k):
            inward(k).wait_send()

            @pl.when(early(k))
            def _():
                for i in range(1, wide):
                    here(k, i).wait_send()
                    relay_out(k, i).wait_send()

            pltpu.make_async_copy(
                out_ref.at[chunk(k)], out_ref.at[chunk(k)], o_recv.at[k]
            ).wait()

        for near_too in (False, True):
            for t in range(strips):
                for i in range(half):
                    each_depth(lambda d: g_copy(near_too, i, t, d).wait_send())

    for t in range(strips):
        for i, j in layer_mates:
            share(t, i, j).wait_send()


def shards(gate_pre, up_pre, out_grad, n_node, n_local):
    wide, layers, tall = n_node // n_local, n_local // 2, n_local // 2
    tokens, units = gate_pre.shape
    width = out_grad.shape[1] // wide
    count = units // TILE
    strips = strips_of(width)
    slots = layers * wide
    half = gate_pre.dtype
    dma = pltpu.SemaphoreType.DMA
    result = pl.pallas_call(
        functools.partial(kernel, n_node, n_local),
        out_shape=OUT((units, width), half),
        in_specs=[pl.BlockSpec(memory_space=pl.ANY)] * 3,
        out_specs=pl.BlockSpec(memory_space=pltpu.VMEM),
        scratch_shapes=[
            pltpu.VMEM((tokens, units), half),
            pltpu.VMEM((tokens, units), half),
            pltpu.VMEM((tokens, wide * width), half),
            pltpu.VMEM((slots * tokens, units), half),
            pltpu.VMEM((2 * layers, slots * tokens, width), half),
            pltpu.VMEM((layers, units, width), half),
            pltpu.VMEM((layers, units, width), half),
            pltpu.VMEM((layers - 1, units, width), half),
            dma((count, 2)),
            dma,
            dma((strips, wide * tall)),
            dma((tall, strips, wide)),
            dma((tall, strips, layers - 1, 2)),
            dma((tall, strips, 2)),
            dma((count, slots)),
            dma((count, slots)),
            dma((count, layers, 2)),
            dma((count, layers - 1)),
            dma((count,)),
        ],
        compiler_params=pltpu.CompilerParams(
            collective_id=0, has_side_effects=True, vmem_limit_bytes=62 * 1024 * 1024
        ),
    )(gate_pre, up_pre, out_grad)
    return result.astype(jnp.float32)


OUT = jax.ShapeDtypeStruct


def solution(mesh):
    placed = (P("node", "local"), P("node", "local"), P("node", "local"))
    return jax.shard_map(
        functools.partial(shards, n_node=mesh.shape["node"], n_local=mesh.shape["local"]),
        mesh=mesh,
        in_specs=placed,
        out_specs=P("local", "node"),
        check_vma=False,
    )
```

```python
import functools

import jax
import jax.numpy as jnp
from jax import lax
from jax.experimental import pallas as pl
from jax.experimental.pallas import tpu as pltpu
from jax.sharding import PartitionSpec as P

TILE = 128
LAG = 12
EARLY = 4
RAMP = 0
DEPTH = 2
STRIPS = 4


def strips_of(width):
    return next(n for n in (STRIPS, 2, 1) if width % (n * TILE) == 0)


def kernel(
    n_node, n_local, gate_hbm, up_hbm, grad_hbm, out_ref,
    gate, up, own, hidden, grads, going, coming, giving,
    in_sem, own_sem, l_send, l_recv, g_sem, twin_sem, h_send, h_recv, p_sem, o_send, o_recv,
):
    wide, deep, tall = n_node // n_local, n_local, n_local // 2
    layers = deep // 2
    node, local = lax.axis_index("node"), lax.axis_index("local")
    z, x, y, c = node // wide, node % wide, local // 2, local % 2
    side = z // layers
    tokens, units = gate.shape
    width = out_ref.shape[1]
    count = units // TILE
    strips = strips_of(width)
    strip = width // strips
    slots = layers * wide
    averaging = 1.0 / n_node

    def depth(zz):
        return jnp.where(zz < layers, layers - 1 - zz, zz - layers)

    def layer(half, d):
        return jnp.where(half == 0, layers - 1 - d, layers + d)

    mine = depth(z)
    inside = mine == 0
    outside = jnp.logical_not(inside)
    inner_z = layer(side, 0)
    mirror = (layer(1 - side, 0) * wide + x, local)
    twin = (node, y * 2 + 1 - c)

    def device(zz, xx, yy, cc):
        return (zz * wide + xx, yy * 2 + cc)

    def beside(i):
        return (x + i) % wide

    def slot_of(d, xx):
        return d * wide + xx

    my_slot = slot_of(mine, x)

    def rows(slot):
        return pl.ds(pl.multiple_of(slot * tokens, 16), tokens)

    def chunk(k):
        return pl.ds(pl.multiple_of(k * TILE, TILE), TILE)

    def remote(source, target, send, recv, where):
        return pltpu.make_async_remote_copy(
            src_ref=source, dst_ref=target, send_sem=send, recv_sem=recv,
            device_id=where, device_id_type=pl.DeviceIdType.MESH,
        )

    def loads(k):
        return [
            pltpu.make_async_copy(gate_hbm.at[:, chunk(k)], gate.at[:, chunk(k)], in_sem.at[k, 0]),
            pltpu.make_async_copy(up_hbm.at[:, chunk(k)], up.at[:, chunk(k)], in_sem.at[k, 1]),
        ]

    own_load = pltpu.make_async_copy(grad_hbm, own, own_sem)
    own_load.start()
    for copy in loads(0):
        copy.start()

    @pl.loop(1, count)
    def _(k):
        for copy in loads(k):
            copy.start()

    barrier = pltpu.get_barrier_semaphore()

    def greet(target):
        pl.semaphore_signal(
            barrier, inc=1, device_id=target, device_id_type=pl.DeviceIdType.MESH
        )

    ring = [(i, j, m) for i in range(wide) for j in range(tall) for m in range(2)]

    @pl.when(inside)
    def _():
        greet(mirror)
        for d in range(layers):
            for i, j, m in ring:
                if (d, i, j, m) != (0, 0, 0, 0):
                    greet(device(layer(side, d), beside(i), (y + j) % tall, (c + m) % 2))
        pl.semaphore_wait(barrier, layers * len(ring))

    layer_mates = [(i, j) for i in range(wide) for j in range(tall) if (i, j) != (0, 0)]

    @pl.when(outside)
    def _():
        for i, j, m in ring:
            greet(device(inner_z, beside(i), (y + j) % tall, (c + m) % 2))
        for i, j in layer_mates:
            greet(device(z, beside(i), (y + j) % tall, c))
        pl.semaphore_wait(barrier, len(ring) + len(layer_mates))

    half = tall // 2

    def row_of(near, i):
        low, high = i, tall - 1 - i
        return jnp.where((side == 0) == near, low, high)

    def entry(near, i, cc):
        return (layers if near else 0) + depth(row_of(near, i) * 2 + cc)

    own_near = jnp.where(y >= half, 1, 0) == side
    own_low = y < half
    own_at = jnp.where(own_near, half, 0) + jnp.where(own_low, y, tall - 1 - y)
    own_entry = jnp.where(own_near, layers, 0) + depth(y * 2 + c)

    def share_source(t, i, held):
        return held.at[:, pl.ds(pl.multiple_of(beside(i) * width + t * strip, TILE), strip)]

    def share_target(t):
        return grads.at[own_entry, rows(my_slot), pl.ds(t * strip, strip)]

    def share(t, i, j):
        return remote(
            share_source(t, i, own), share_target(t), l_send.at[t, i * tall + j], l_recv.at[own_at, t, x],
            device(z, beside(i), (y + j) % tall, c),
        )

    def keep(t):
        return pltpu.make_async_copy(share_source(t, 0, grad_hbm), share_target(t), l_recv.at[own_at, t, x])

    own_load.wait()
    for t in range(strips):
        for i, j in layer_mates:
            share(t, i, j).start()
    for t in range(strips):
        keep(t).start()

    def layer_rows(d):
        return pl.ds(pl.multiple_of(d * (wide * tokens), 16), wide * tokens)

    def shared(near, i, t):
        for xx in range(wide):
            part = grads.at[entry(near, i, c), rows(slot_of(mine, xx)), pl.ds(t * strip, strip)]
            pltpu.make_async_copy(part, part, l_recv.at[near * half + i, t, xx]).wait()

    def g_copy(near, i, t, d):
        part = grads.at[entry(near, i, c), layer_rows(d), pl.ds(t * strip, strip)]
        at = near * half + i
        return remote(
            part, part, g_sem.at[at, t, d - 1, 0], g_sem.at[at, t, d - 1, 1],
            device(inner_z, x, y, c),
        )

    def each_depth(act):
        for d in range(1, layers):
            @pl.when(mine == d)
            def _():
                act(d)

    def g_start(near, t):
        for i in range(half):
            shared(near, i, t)
            each_depth(lambda d: g_copy(near, i, t, d).start())

    def twin_copy(near, i, t, cc):
        part = grads.at[entry(near, i, cc), :, pl.ds(t * strip, strip)]
        at = near * half + i
        return remote(part, part, twin_sem.at[at, t, 0], twin_sem.at[at, t, 1], twin)

    def g_pass(near, t):
        for i in range(half):
            shared(near, i, t)
            for d in range(1, layers):
                g_copy(near, i, t, d).wait_recv()
            twin_copy(near, i, t, c).start()

    def g_passed(near, t):
        for i in range(half):
            twin_copy(near, i, t, 1 - c).wait_recv()

    step = next(b for b in (128, 112, 96, 64, 32, 16) if tokens % b == 0)

    def activate(k):
        for copy in loads(k):
            copy.wait()
        at = chunk(k)
        for first in range(0, tokens, step):
            g = gate[pl.ds(first, step), at].astype(jnp.float32)
            u = up[pl.ds(first, step), at].astype(jnp.float32)
            value = g * jax.nn.sigmoid(g) * u
            into = pl.ds(pl.multiple_of(my_slot * tokens + first, 16), step)
            hidden[into, at] = value.astype(hidden.dtype)

    def h_copy(k, slot, index, where):
        part = hidden.at[rows(slot), chunk(k)]
        return remote(part, part, h_send.at[k, index], h_recv.at[k, slot], where)

    def here(k, i):
        return h_copy(k, my_slot, i, device(z, beside(i), y, c))

    def inward(k):
        return h_copy(k, my_slot, 0, device(inner_z, x, y, c))

    def relay_out(k, i):
        return h_copy(k, slot_of(mine, beside(i)), wide + i - 1, device(inner_z, x, y, c))

    def relay_in(k, d, i):
        return h_copy(k, slot_of(d, x), d * wide + i, device(z, beside(i), y, c))

    def early(k):
        return k % 3 == 2

    def late(k):
        return k % 3 != 2

    def send_in(k):
        activate(k)
        for i in range(1, wide):
            here(k, i).start()

    def send_out(k):
        activate(k)
        inward(k).start()

        @pl.when(early(k))
        def _():
            for i in range(1, wide):
                here(k, i).start()

    def pass_out(k):
        @pl.when(early(k))
        def _():
            for i in range(1, wide):
                h_copy(k, slot_of(mine, beside(i)), 0, twin).wait_recv()
                relay_out(k, i).start()

    def drain(k):
        inward(k).wait_send()

        @pl.when(early(k))
        def _():
            for i in range(1, wide):
                here(k, i).wait_send()
                relay_out(k, i).wait_send()

    def pass_in(k):
        for d in range(1, layers):
            h_copy(k, slot_of(d, x), 0, twin).wait_recv()

            @pl.when(late(k))
            def _():
                for i in range(1, wide):
                    relay_in(k, d, i).start()

    def gathered(k):
        for d in range(layers):
            for i in range(1, wide):
                h_copy(k, slot_of(d, beside(i)), 0, twin).wait_recv()

    def product(k, index, at):
        return lax.dot_general(
            hidden[:, chunk(k)], grads[index, :, at], (((0,), (0,)), ((), ())),
            preferred_element_type=jnp.float32,
        ) * averaging

    def p_copy(k, index, at):
        return remote(
            going.at[index, chunk(k), at], coming.at[index, chunk(k), at],
            p_sem.at[k, index, 0], p_sem.at[k, index, 1], mirror,
        )

    whole = pl.ds(0, width)

    def lane(t):
        return pl.ds(t * strip, strip)

    def far(k, i, cc, at):
        index = entry(False, i, cc)
        going[index, chunk(k), at] = product(k, index, at).astype(going.dtype)
        p_copy(k, index, at).start()

    def o_copy(k, d):
        return remote(
            giving.at[d - 1, chunk(k)], out_ref.at[chunk(k)],
            o_send.at[k, d - 1], o_recv.at[k], device(layer(side, d), x, y, c),
        )

    def near(k):
        for d in reversed(range(layers)):
            p_copy(k, d, whole).wait_recv()
            total = product(k, layers + d, whole) + coming[d, chunk(k)].astype(jnp.float32)
            if d:
                giving[d - 1, chunk(k)] = total.astype(giving.dtype)
                o_copy(k, d).start()
            else:
                out_ref[chunk(k)] = total.astype(out_ref.dtype)

    first_c = 1 - side

    @pl.when(inside)
    def _():
        send_in(0)
        send_in(1)
        pass_in(0)
        for n in range(EARLY):
            send_in(n + 2)
            if n < strips:
                g_pass(False, n)
            pass_in(n + 1)
            gathered(n)
            for t in range(min(n, strips)):
                for i in range(half):
                    far(n, i, c, lane(t))
                    far(n, i, 1 - c, lane(t))
            if n < strips:
                for k in range(n + 1):
                    for i in range(half):
                        far(k, i, c, lane(n))
                g_passed(False, n)
                for k in range(n + 1):
                    for i in range(half):
                        far(k, i, 1 - c, lane(n))

        def multiply(k):
            gathered(k)
            for i in range(half):
                far(k, i, first_c, whole)
                far(k, i, 1 - first_c, whole)

        @pl.loop(EARLY, EARLY + RAMP)
        def _(k):
            for m in range(2):
                send_in(2 * k - EARLY + 2 + m)
                pass_in(2 * k - EARLY + 1 + m)
            multiply(k)

        def body(k):
            @pl.when(k + RAMP + 2 < count)
            def _():
                send_in(k + RAMP + 2)

            @pl.when(k + RAMP + 1 < count)
            def _():
                pass_in(k + RAMP + 1)

            multiply(k)

        @pl.loop(EARLY + RAMP, LAG)
        def _(k):
            body(k)

        for t in range(strips):
            g_pass(True, t)
        for t in range(strips):
            g_passed(True, t)

        @pl.loop(LAG, count)
        def _(k):
            body(k)
            near(k - LAG)

        @pl.loop(count - LAG, count)
        def _(k):
            near(k)

        @pl.loop(0, count)
        def _(k):
            for i in range(1, wide):
                here(k, i).wait_send()

            @pl.when(late(k))
            def _():
                for d in range(1, layers):
                    for i in range(1, wide):
                        relay_in(k, d, i).wait_send()

            for d in range(layers):
                p_copy(k, d, whole).wait_send()
            for d in range(1, layers):
                o_copy(k, d).wait_send()

        for near_too in (False, True):
            for t in range(strips):
                for i in range(half):
                    twin_copy(near_too, i, t, c).wait_send()

    @pl.when(outside)
    def _():
        send_out(0)
        for n in range(EARLY):
            if n < strips:
                g_start(False, n)
            if n + 1 >= DEPTH:
                drain(n + 1 - DEPTH)
            send_out(n + 1)
            pass_out(n)

        @pl.loop(EARLY + 1, count)
        def _(k):
            for t in range(strips):
                @pl.when(k == EARLY + 1 + t)
                def _():
                    g_start(True, t)

            drain(k - DEPTH)
            send_out(k)
            pass_out(k - 1)

        pass_out(count - 1)

        @pl.loop(count - DEPTH, count)
        def _(k):
            drain(k)

        @pl.loop(0, count)
        def _(k):
            pltpu.make_async_copy(
                out_ref.at[chunk(k)], out_ref.at[chunk(k)], o_recv.at[k]
            ).wait()

        for near_too in (False, True):
            for t in range(strips):
                for i in range(half):
                    each_depth(lambda d: g_copy(near_too, i, t, d).wait_send())

    for t in range(strips):
        for i, j in layer_mates:
            share(t, i, j).wait_send()


def shards(gate_pre, up_pre, out_grad, n_node, n_local):
    wide, layers, tall = n_node // n_local, n_local // 2, n_local // 2
    tokens, units = gate_pre.shape
    width = out_grad.shape[1] // wide
    count = units // TILE
    strips = strips_of(width)
    slots = layers * wide
    half = gate_pre.dtype
    dma = pltpu.SemaphoreType.DMA
    result = pl.pallas_call(
        functools.partial(kernel, n_node, n_local),
        out_shape=OUT((units, width), half),
        in_specs=[pl.BlockSpec(memory_space=pl.ANY)] * 3,
        out_specs=pl.BlockSpec(memory_space=pltpu.VMEM),
        scratch_shapes=[
            pltpu.VMEM((tokens, units), half),
            pltpu.VMEM((tokens, units), half),
            pltpu.VMEM((tokens, wide * width), half),
            pltpu.VMEM((slots * tokens, units), half),
            pltpu.VMEM((2 * layers, slots * tokens, width), half),
            pltpu.VMEM((layers, units, width), half),
            pltpu.VMEM((layers, units, width), half),
            pltpu.VMEM((layers - 1, units, width), half),
            dma((count, 2)),
            dma,
            dma((strips, wide * tall)),
            dma((tall, strips, wide)),
            dma((tall, strips, layers - 1, 2)),
            dma((tall, strips, 2)),
            dma((count, slots)),
            dma((count, slots)),
            dma((count, layers, 2)),
            dma((count, layers - 1)),
            dma((count,)),
        ],
        compiler_params=pltpu.CompilerParams(
            collective_id=0, has_side_effects=True, vmem_limit_bytes=56 * 1024 * 1024
        ),
    )(gate_pre, up_pre, out_grad)
    return result.astype(jnp.float32)


OUT = pltpu.VMEM


def solution(mesh):
    placed = (P("node", "local"), P("node", "local"), P("node", "local"))
    return jax.shard_map(
        functools.partial(shards, n_node=mesh.shape["node"], n_local=mesh.shape["local"]),
        mesh=mesh,
        in_specs=placed,
        out_specs=P("local", "node"),
        check_vma=False,
    )
```
